32 devices in a mesh: dp: 2 (over x), pz: 4 (over z), py: 4 (over y, core).
Axes of the slice: x: 2, y: 2, z: 4, core: 2. Of those that a mesh axis runs over, the one named last changes fastest.
Arguments:
- rho_re: float32 [4, 240, 240, 240], P('dp', None, 'py', 'pz'), parts along dimension 0
- rho_im: float32 [4, 240, 240, 240], P('dp', None, 'py', 'pz'), parts along dimension 0
- g_re: float32 [240, 240, 240], P('py', 'pz')
- g_im: float32 [240, 240, 240], P('py', 'pz')
Outputs:
- output 1: float32 [4, 240, 240, 240], P('dp', None, 'py', 'pz'), parts along dimension 0
- output 2: float32 [4, 240, 240, 240], P('dp', None, 'py', 'pz'), parts along dimension 0
- output 3: float32 [4, 240, 240, 240], P('dp', 'py', 'pz'), parts along dimension 0
- output 4: float32 [4, 240, 240, 240], P('dp', 'py', 'pz'), parts along dimension 0
There are 2 independent parts. The reference program is written for one: setup_inputs(seed, part) draws one part's arguments, and reference() takes and returns one part's arrays. A program takes and returns all parts, laid end to end along the dimension named above; an argument that names none is the same for every part.
All inputs are finite; a program needn't handle non-finite values.
Results may differ from the reference program's by a relative error of at most 0.001.
Values sent between devices are 32-bit elements.
A program may use at most 1 GiB of HBM per device.

```python
import jax
import jax.numpy as jnp
from jax import lax

GRID = 240
FIELDS = 2


def green_kernel():
    positions = jnp.arange(GRID)
    wavenum = jnp.where(positions < (GRID + 1) // 2, positions, positions - GRID).astype(jnp.float32)
    wave_sq = wavenum * wavenum * (16.0 / (GRID * GRID))
    return 1.0 / (1.0 + wave_sq[:, None, None] + 2.0 * wave_sq[None, :, None] + 3.0 * wave_sq[None, None, :])


def setup_inputs(seed: int = 0, part: int = 0) -> dict:
    part_key = jax.random.fold_in(jax.random.key(seed), part)
    key_re, key_im = jax.random.split(part_key)
    field_shape = (FIELDS, GRID, GRID, GRID)
    rho_re = jax.random.normal(key_re, field_shape, jnp.float32)
    rho_im = jax.random.normal(key_im, field_shape, jnp.float32)
    green_re_key, green_im_key = jax.random.split(jax.random.key(seed + 1))
    kernel = green_kernel()
    g_re = kernel * (1.0 + 0.5 * jax.random.normal(green_re_key, kernel.shape, jnp.float32))
    g_im = kernel * (0.5 * jax.random.normal(green_im_key, kernel.shape, jnp.float32))
    return {"rho_re": rho_re, "rho_im": rho_im, "g_re": g_re, "g_im": g_im}


def reference(rho_re, rho_im, g_re, g_im):
    green_fn = lax.complex(g_re, g_im)

    def one_field(field_pair):
        volume = lax.complex(field_pair[0], field_pair[1])
        spectrum = jnp.fft.fftn(volume, axes=(0, 1, 2), norm="ortho") * green_fn
        restored = jnp.fft.ifftn(spectrum, axes=(0, 1, 2), norm="ortho")
        return jnp.real(restored), jnp.imag(restored), jnp.real(spectrum), jnp.imag(spectrum)

    phi_re, phi_im, hat_re, hat_im = lax.map(one_field, (rho_re, rho_im))
    return (phi_re, phi_im, hat_re, hat_im)
```

```python
import functools

import jax
import jax.numpy as jnp
import numpy as np
from jax import lax
from jax.experimental import pallas as pl
from jax.experimental.pallas import tpu as pltpu
from jax.sharding import PartitionSpec as P


N = 240
B = 60
S = 64
CHUNKS = (12, 24, 24)
FIRST = (0, 12, 36)
PLACE = (0, 16, 40)
VMEM_LIMIT = 60 * 1024 * 1024


def dft(sign):
    k = np.arange(N)
    return np.exp(sign * 2j * np.pi * ((k[:, None] * k[None, :]) % N) / N) / np.sqrt(N)


def thirds(w):
    w = w.astype(np.float64)
    out = []
    for _ in range(3):
        part = w.astype(jnp.bfloat16)
        out.append(part)
        w = w - part.astype(np.float64)
    return out


def spread(kind):
    i = np.arange(N)
    if kind == "plain":
        return i
    if kind == "block":
        return (i // B) * S + i % B
    local = i % B
    place = np.select([local < 12, local < 36], [local, local + 4], local + 4)
    return (i // B) * S + place


def left_matrix(sign, out_kind, in_kind):
    w = dft(sign)
    rows, cols = spread(out_kind), spread(in_kind)
    full = np.zeros((256, 256), np.complex128)
    full[np.ix_(rows, cols)] = w
    both = np.stack([full.real.reshape(4, S, 256), full.imag.reshape(4, S, 256)], axis=1).reshape(512, 256)
    a, b, c = thirds(both)
    return np.concatenate([a, b, c, a, b, a], axis=1)


def right_matrix(sign):
    w = dft(sign)
    z = (np.arange(N) // B) * 128 + np.arange(N) % B
    k = np.arange(N)
    if sign < 0:
        full = np.zeros((512, 512))
        full[np.ix_(z, k)] = w.real
        full[np.ix_(z, 256 + k)] = w.imag
        full[np.ix_(S + z, k)] = -w.imag
        full[np.ix_(S + z, 256 + k)] = w.real
    else:
        full = np.zeros((512, 512))
        full[np.ix_(k, z)] = w.real
        full[np.ix_(k, S + z)] = w.imag
        full[np.ix_(256 + k, z)] = -w.imag
        full[np.ix_(256 + k, S + z)] = w.real
    a, b, c = thirds(full)
    return np.concatenate([a, b, c, a, b, a], axis=0)


def split3(x):
    a = x.astype(jnp.bfloat16)
    r = x - a.astype(jnp.float32)
    b = r.astype(jnp.bfloat16)
    c = (r - b.astype(jnp.float32)).astype(jnp.bfloat16)
    return a, b, c


def sign_lanes(rows):
    lane = lax.broadcasted_iota(jnp.int32, (rows, 128), 1)
    return jnp.where(lane < S, -1.0, 1.0).astype(jnp.float32)


def left_product(w_ref, x_ref, s_ref, r_ref):
    a, b, c = split3(x_ref[...])
    for place, part in enumerate((a, a, a, b, b, c)):
        s_ref[place * 256:(place + 1) * 256, :] = part
    r_ref[...] = jnp.dot(w_ref[...], s_ref[...], preferred_element_type=jnp.float32)


def block_of(r_ref, block, k, sgn):
    start = pl.multiple_of(block * 128, 128)
    lanes = slice(k * 128, (k + 1) * 128)
    real = r_ref[pl.ds(start, S), lanes]
    imag = r_ref[pl.ds(start + S, S), lanes]
    return real + pltpu.roll(imag, S, 1) * sgn


def x_forward(me_ref, re_ref, im_ref, w_ref, *rest):
    outs, (x_ref, s_ref, r_ref) = rest[:12], rest[12:]
    step = pl.program_id(0)
    py = me_ref[0]

    @pl.when(step == 0)
    def _():
        x_ref[...] = jnp.zeros_like(x_ref)

    sgn = sign_lanes(S)

    def half(h):
        for k in range(4):
            x_ref[0:N, k * 128:k * 128 + B] = re_ref[0, :, h * 4 + k, :]
            x_ref[0:N, k * 128 + S:k * 128 + S + B] = im_ref[0, :, h * 4 + k, :]
        left_product(w_ref, x_ref, s_ref, r_ref)
        for s in range(4):
            block = jnp.bitwise_xor(py, s)
            for k in range(4):
                y = step * 8 + h * 4 + k
                value = block_of(r_ref, block, k, sgn)
                for c, size in enumerate(CHUNKS):
                    outs[c * 4 + s][pl.ds(y, size, stride=B), :] = value[PLACE[c]:PLACE[c] + size]

    half(0)

    @pl.when(step < 7)
    def _():
        half(1)


def x_inverse(me_ref, *rest):
    pieces, rest = rest[:12], rest[12:]
    w_ref, rest = rest[0], rest[1:]
    re_ref, im_ref, x_ref, s_ref, r_ref = rest[-5:]
    step = pl.program_id(0)
    py = me_ref[0]

    @pl.when(step == 0)
    def _():
        x_ref[...] = jnp.zeros_like(x_ref)

    sgn = sign_lanes(S)

    def half(h):
        for s in range(4):
            base = jnp.bitwise_xor(py, s) * S
            for k in range(4):
                y = step * 8 + h * 4 + k
                for c, size in enumerate(CHUNKS):
                    rows = pl.ds(pl.multiple_of(base + PLACE[c], 8), size)
                    x_ref[rows, k * 128:(k + 1) * 128] = pieces[c * 4 + s][pl.ds(y, size, stride=B), :]
        left_product(w_ref, x_ref, s_ref, r_ref)
        for k in range(4):
            for b in range(4):
                size = S if b < 3 else N - 3 * S
                value = block_of(r_ref, b, k, sgn)
                re_ref[0, b * S:b * S + size, h * 4 + k, :] = value[:size, :B]
                im_ref[0, b * S:b * S + size, h * 4 + k, :] = pltpu.roll(value, S, 1)[:size, :B]

    half(0)

    @pl.when(step < 7)
    def _():
        half(1)


def y_transform(forward, me_ref, *rest):
    pieces, w_ref, outs, (x_ref, s_ref, r_ref) = rest[:4], rest[4], rest[5:9], rest[9:]
    py, pz = me_ref[0], me_ref[1]

    @pl.when(pl.program_id(0) == 0)
    def _():
        x_ref[...] = jnp.zeros_like(x_ref)

    sgn = sign_lanes(S)
    for s in range(4):
        source = jnp.bitwise_xor(py, s) if forward else lax.rem(pz + 4 - s, 4)
        rows = pl.ds(pl.multiple_of(source * S, S), B)
        for k in range(4):
            x_ref[rows, k * 128:(k + 1) * 128] = pieces[s][k * B:(k + 1) * B, :]
    left_product(w_ref, x_ref, s_ref, r_ref)
    for s in range(4):
        dest = lax.rem(pz + s, 4) if forward else jnp.bitwise_xor(py, s)
        for k in range(4):
            outs[s][k * B:(k + 1) * B, :] = block_of(r_ref, dest, k, sgn)[:B]


def z_transform(group, me_ref, *rest):
    pieces, (g_re, g_im, w_ref, v_ref) = rest[:4], rest[4:8]
    outs, hat_re, hat_im, x_ref, s_ref, r_ref = rest[-9:-5], rest[-5], rest[-4], rest[-3], rest[-2], rest[-1]
    pz = me_ref[1]

    @pl.when(pl.program_id(0) == 0)
    def _():
        x_ref[...] = jnp.zeros_like(x_ref)

    def product(m_ref):
        a, b, c = split3(x_ref[...])
        for place, part in enumerate((a, a, a, b, b, c)):
            s_ref[:, place * 512:(place + 1) * 512] = part
        r_ref[...] = jnp.dot(s_ref[...], m_ref[...], preferred_element_type=jnp.float32)

    for s in range(4):
        lanes = pl.ds(pl.multiple_of(lax.rem(pz + 4 - s, 4) * 128, 128), 128)
        for k in range(group):
            x_ref[k * S:k * S + B, lanes] = pieces[s][k * B:(k + 1) * B, :]
    product(w_ref)
    for k in range(group):
        re, im = r_ref[k * S:k * S + B, 0:N], r_ref[k * S:k * S + B, 256:256 + N]
        gr, gi = g_re[k], g_im[k]
        hr, hi = re * gr - im * gi, re * gi + im * gr
        hat_re[0, k], hat_im[0, k] = hr, hi
        x_ref[k * S:k * S + B, 0:N] = hr
        x_ref[k * S:k * S + B, N:256] = jnp.zeros((B, 256 - N), jnp.float32)
        x_ref[k * S:k * S + B, 256:256 + N] = hi
        x_ref[k * S:k * S + B, 256 + N:512] = jnp.zeros((B, 256 - N), jnp.float32)
    product(v_ref)
    for s in range(4):
        lanes = pl.ds(pl.multiple_of(lax.rem(pz + s, 4) * 128, 128), 128)
        for k in range(group):
            outs[s][k * B:(k + 1) * B, :] = r_ref[k * S:k * S + B, lanes]


def params(steps):
    return pltpu.CompilerParams(dimension_semantics=("arbitrary",), vmem_limit_bytes=VMEM_LIMIT)


def whole(shape):
    return pl.BlockSpec(shape, lambda i, me: (0,) * len(shape))


LEFT_SCRATCH = [pltpu.VMEM((256, 512), jnp.float32), pltpu.VMEM((1536, 512), jnp.bfloat16),
                pltpu.VMEM((512, 512), jnp.float32)]


def left_cost(steps, rows):
    return pl.CostEstimate(flops=steps * 2 * 512 * 1536 * 512, bytes_accessed=2 * rows * 512, transcendentals=0)


def piece(c):
    return jax.ShapeDtypeStruct((CHUNKS[c] * B, 128), jnp.float32)


def call_x_forward(me, f, re, im, w):
    field = pl.BlockSpec((1, N, 8, B), lambda i, me: (f, 0, i, 0))
    shapes = [piece(c) for c in range(3) for _ in range(4)]
    return pl.pallas_call(
        x_forward, name=f"x_forward_{f}",
        grid_spec=pltpu.PrefetchScalarGridSpec(
            num_scalar_prefetch=1, grid=(8,),
            in_specs=[field, field, whole(w.shape)], out_specs=[whole(s.shape) for s in shapes],
            scratch_shapes=LEFT_SCRATCH),
        out_shape=shapes, compiler_params=params(8), cost_estimate=left_cost(15, 40000))(me, re, im, w)


def call_x_inverse(me, f, pieces, w, before):
    field = pl.BlockSpec((1, N, 8, B), lambda i, me: (f, 0, i, 0))
    whole_field = jax.ShapeDtypeStruct((2, N, B, B), jnp.float32)
    extra = [] if before is None else list(before)
    return pl.pallas_call(
        x_inverse, name=f"x_inverse_{f}",
        grid_spec=pltpu.PrefetchScalarGridSpec(
            num_scalar_prefetch=1, grid=(8,),
            in_specs=[whole(p.shape) for p in pieces] + [whole(w.shape)]
            + [pl.BlockSpec(memory_space=pl.ANY) for _ in extra],
            out_specs=[field, field], scratch_shapes=LEFT_SCRATCH),
        out_shape=[whole_field, whole_field],
        input_output_aliases={} if before is None else {14: 0, 15: 1},
        compiler_params=params(8), cost_estimate=left_cost(15, 40000))(me, *pieces, w, *extra)


def call_y(me, forward, c, pieces, w):
    steps = CHUNKS[c] // 4
    rows = pl.BlockSpec((4 * B, 128), lambda i, me: (i, 0))
    return pl.pallas_call(
        functools.partial(y_transform, forward), name=f"y_{'forward' if forward else 'inverse'}_{c}",
        grid_spec=pltpu.PrefetchScalarGridSpec(
            num_scalar_prefetch=1, grid=(steps,),
            in_specs=[rows] * 4 + [whole(w.shape)], out_specs=[rows] * 4, scratch_shapes=LEFT_SCRATCH),
        out_shape=[piece(c)] * 4, compiler_params=params(steps),
        cost_estimate=left_cost(steps, CHUNKS[c] * 240))(me, *pieces, w)


def call_z(me, f, c, pieces, g_re, g_im, w, v, before):
    group = 12
    steps = CHUNKS[c] // group
    rows = pl.BlockSpec((group * B, 128), lambda i, me: (i, 0))
    first = FIRST[c] // group
    green = pl.BlockSpec((group, B, N), lambda i, me: (first + i, 0, 0))
    hat = pl.BlockSpec((1, group, B, N), lambda i, me: (f, first + i, 0, 0))
    hat_shape = jax.ShapeDtypeStruct((2, B, B, N), jnp.float32)
    extra = [] if before is None else list(before)
    out = pl.pallas_call(
        functools.partial(z_transform, group), name=f"z_{f}_{c}",
        grid_spec=pltpu.PrefetchScalarGridSpec(
            num_scalar_prefetch=1, grid=(steps,),
            in_specs=[rows] * 4 + [green] * 2 + [whole(w.shape)] * 2
            + [pl.BlockSpec(memory_space=pl.ANY) for _ in extra],
            out_specs=[rows] * 4 + [hat] * 2,
            scratch_shapes=[pltpu.VMEM((group * S, 512), jnp.float32), pltpu.VMEM((group * S, 3072), jnp.bfloat16),
                            pltpu.VMEM((group * S, 512), jnp.float32)]),
        out_shape=[piece(c)] * 4 + [hat_shape] * 2,
        input_output_aliases={} if before is None else {9: 4, 10: 5},
        compiler_params=params(steps),
        cost_estimate=pl.CostEstimate(flops=steps * 2 * 2 * 768 * 3072 * 512, bytes_accessed=steps * 8 << 20,
                                      transcendentals=0))(me, *pieces, g_re, g_im, w, v, *extra)
    return out[:4], out[4:]


def exchange(pieces, axis):
    moved = [pieces[0]]
    for s in range(1, 4):
        route = [(i, i ^ s if axis == "py" else (i + s) % 4) for i in range(4)]
        moved.append(lax.ppermute(pieces[s], axis, route))
    return moved


ORDER = [(0, 0), (0, 1), (0, 2), (1, 1), (1, 2), (1, 0)]


def solution(mesh):
    w_x = left_matrix(-1, "chunk", "plain")
    v_x = left_matrix(1, "plain", "chunk")
    w_y = left_matrix(-1, "block", "block")
    v_y = left_matrix(1, "block", "block")
    w_z, v_z = right_matrix(-1), right_matrix(1)

    def local_solve(rho_re, rho_im, g_re, g_im):
        me = jnp.stack([lax.axis_index("py"), lax.axis_index("pz")]).astype(jnp.int32)
        wx, vx, wy, vy, wz, vz = (jnp.asarray(m) for m in (w_x, v_x, w_y, v_y, w_z, v_z))
        first = [call_x_forward(me, f, rho_re, rho_im, wx) for f in range(2)]
        back = {}
        hat = phi = None
        for f, c in ORDER:
            pieces = exchange(first[f][c * 4:c * 4 + 4], "py")
            pieces = exchange(call_y(me, True, c, pieces, wy), "pz")
            pieces, hat = call_z(me, f, c, pieces, g_re, g_im, wz, vz, hat)
            pieces = exchange(pieces, "pz")
            back[f, c] = exchange(call_y(me, False, c, pieces, vy), "py")
        for f in range(2):
            pieces = [p for c in range(3) for p in back[f, c]]
            phi = call_x_inverse(me, f, pieces, vx, phi)
        return phi[0], phi[1], hat[0], hat[1]

    space_layout = P("dp", None, "py", "pz")
    wave_layout = P("dp", "py", "pz", None)
    green_layout = P("py", "pz", None)
    return jax.shard_map(local_solve, mesh=mesh,
                         in_specs=(space_layout, space_layout, green_layout, green_layout),
                         out_specs=(space_layout, space_layout, wave_layout, wave_layout),
                         check_vma=False)
```
